128 devices in a mesh: lat: 16 (over z, y_lo, core), lon: 8 (over y_hi, x).
Axes of the slice: x: 4, y: 4 (y_hi: 2, y_lo: 2; y = y_hi * 2 + y_lo), z: 4, core: 2. Of those that a mesh axis runs over, the one named last changes fastest.
Arguments:
- field: bfloat16 [256, 256, 256], P('lat', 'lon'), may hold values from -6 to 6
- weights: bfloat16 [16, 8, 3072, 3072], P('lat', 'lon'), may hold values from -0.09375 to 0.09375
- strip_ids: int32 [16, 8], P('lat'), may hold values from 0 to 63, as said below
- counts: int32 [16], P('lat'), may hold values from 2 to 8, as said below
Outputs:
- remapped: bfloat16 [131072, 256], P(('lat', 'lon'))
The draws below stay inside these ranges and needn't reach their ends.
Inputs may be any that keep to these rules, and one draw needn't show every extreme that they name: `strip_ids`: row b holds consecutive global strip numbers, the last one repeated where the run meets the end of its window, all among the strips of source bands b - 2 to b + 2, band c holding strips 4 * c to 4 * c + 3. Band b uses the first counts[b] slots of its row.
All inputs are finite; a program needn't handle non-finite values.
Results may differ from the reference program's by a relative error of at most 0.0059.
Values may be sent and summed in bfloat16 or wider, within the bound.
No kernel may reach another device: no remote copies, remote signals or barrier semaphores. Data moves between devices by JAX's collectives and lax.ppermute only.
A program may use at most 64 MiB of HBM per device.

```python
import jax
import jax.numpy as jnp
from jax import lax

CHANNELS = 256
SRC_ROWS = 16
SRC_LON = 32
STRIP_ROWS = 4
STRIP_CELLS = 128
SLOTS = 8
REACH = 2
TGT_DEV = 1024
TGT_WIN = 3072
NUM_LAT = 256
NUM_LON = 256
NUM_TGT = 131072
N_LAT = 16
N_LON = 8


def strip_plan(key):
    per_device = SRC_ROWS // STRIP_ROWS
    strip_total = N_LAT * per_device
    band_index = jnp.arange(N_LAT, dtype=jnp.int32)
    lower = jnp.maximum(0, (band_index - REACH) * per_device)
    upper = jnp.minimum(strip_total, (band_index + REACH + 1) * per_device)
    drawn = jax.random.randint(jax.random.fold_in(key, 11), (N_LAT,), 2, SLOTS + 1)
    pattern = band_index % 4
    forced = (pattern == 0) | (pattern == 2)
    used = jnp.where(forced, SLOTS, drawn)
    room = upper - lower - used + 1
    offset = jax.random.randint(jax.random.fold_in(key, 12), (N_LAT,), 0, room)
    first_strip = lower + offset
    first_strip = jnp.where(pattern == 0, lower, jnp.where(pattern == 2, upper - SLOTS, first_strip))
    slot_range = jnp.arange(SLOTS, dtype=jnp.int32)
    chosen = jnp.minimum(first_strip[:, None] + slot_range[None, :], upper[:, None] - 1)
    return (chosen.astype(jnp.int32), used.astype(jnp.int32))


def draw_strip_ids(key, part):
    return strip_plan(key)[0]


def draw_counts(key, part):
    return strip_plan(key)[1]


def level_of(own_key, dims, shards, least, top_value):
    level, own = 1.0, jax.random.fold_in(own_key, 6)
    for position, parts in shards:
        draws = jnp.exp(jax.random.uniform(jax.random.fold_in(own, position), (parts,), jnp.float32, least / len(shards), top_value / len(shards)))
        level = level * jnp.repeat(draws, dims[position] // parts).reshape([-1 if axis == position else 1 for axis in range(len(dims))])
    return level


def normal_values(stream_key, shape, deviation, limit, shards=(), kind=jnp.bfloat16):
    values = jax.random.normal(stream_key, shape, jnp.float32) * deviation
    if len(shards) > 0:
        values = level_of(stream_key, shape, shards, -0.22, 0.18) * values
    return jnp.clip(values, min=-limit, max=limit).astype(kind)


def setup_inputs(seed: int = 0) -> dict:
    seeds = jax.random.split(jax.random.key(seed), 5)
    return {
        "field": normal_values(seeds[0], (NUM_LAT, NUM_LON, CHANNELS), 1.0, 6.0, ((0, 16), (1, 8))),
        "weights": normal_values(seeds[1], (N_LAT, N_LON, TGT_WIN, SLOTS * 3 * STRIP_CELLS), (3 * STRIP_CELLS * SLOTS * 3 // 2) ** -0.5, 0.09375, ((0, 16), (1, 8))),
        "strip_ids": draw_strip_ids(jax.random.fold_in(seeds[4], 71), 0),
        "counts": draw_counts(jax.random.fold_in(seeds[4], 71), 0),
    }


def reference(field, weights, strip_ids, counts):
    lon_wrapped = jnp.concatenate([field[:, -1:], field, field[:, :1]], axis=1)
    padded = jnp.concatenate([lon_wrapped[:1], lon_wrapped, lon_wrapped[-1:]], axis=0)
    values = padded.astype(jnp.float32)
    eastward = ((values[1:-1, 2:] - values[1:-1, :-2]) * 0.5).astype(jnp.bfloat16)
    northward = ((values[2:, 1:-1] - values[:-2, 1:-1]) * 0.5).astype(jnp.bfloat16)
    strip_total = NUM_LAT // STRIP_ROWS

    def sectorize(component):
        shaped = component.reshape(strip_total, STRIP_ROWS, N_LON, SRC_LON, CHANNELS)
        return shaped.transpose(0, 2, 1, 3, 4).reshape(strip_total, N_LON, STRIP_CELLS, CHANNELS)

    strips = jnp.stack([sectorize(field), sectorize(eastward), sectorize(northward)], axis=2)
    strips = strips.reshape(strip_total, N_LON, 3 * STRIP_CELLS, CHANNELS)
    slot_range = jnp.arange(SLOTS, dtype=jnp.int32)

    def band_rows(band_index):
        chosen = jnp.take(strips, strip_ids[band_index].astype(jnp.int32), axis=0)
        live_slots = slot_range < counts[band_index]
        chosen = jnp.where(live_slots[:, None, None, None], chosen, jnp.zeros_like(chosen))
        chosen = chosen.transpose(1, 0, 2, 3).reshape(N_LON, SLOTS * 3 * STRIP_CELLS, CHANNELS)
        weights_band = weights[band_index]

        def sector_partial(sector, collected):
            result = jnp.dot(weights_band[sector], chosen[sector], preferred_element_type=jnp.float32)
            return collected.at[sector].set(result)

        collected = lax.fori_loop(0, N_LON, sector_partial, jnp.zeros((N_LON, TGT_WIN, CHANNELS), jnp.float32))
        blocks = collected.reshape(N_LON, 3, TGT_DEV, CHANNELS)
        total = blocks[:, 1] + jnp.roll(blocks[:, 2], 1, axis=0) + jnp.roll(blocks[:, 0], -1, axis=0)
        return total.astype(jnp.bfloat16)

    mapped = lax.map(band_rows, jnp.arange(N_LAT, dtype=jnp.int32))
    return mapped.reshape(NUM_TGT, CHANNELS)
```

```python
import jax
import jax.numpy as jnp
from jax import lax
from jax.experimental import pallas as pl
from jax.experimental.pallas import tpu as pltpu
from jax.sharding import PartitionSpec as P

STRIP_ROWS = 4
SLOTS = 8
REACH = 2
BF16 = jnp.bfloat16
F32 = jnp.float32


def swap(block, axis, partner):
    return lax.ppermute(block, axis, [(i, partner(i)) for i in range(lax.axis_size(axis))])


def near_chip(i):
    return i ^ 2


def far_chip(i, count=16):
    return (i + 2) % count if (i // 2) % 2 else (i - 2) % count


def load_body(meta, w, out, sem, *, which):
    size = out.shape[0]
    start = (jnp.where(meta[1] == 0, 0, 2 * size), jnp.where(meta[1] == 0, 2 * size, 0), size)[which]
    copy = pltpu.make_async_copy(w.at[pl.ds(start, size)], out, sem)
    copy.start()
    copy.wait()


def prep_body(meta, own, near, far, mate, beyond, own_cols, near_cols, far_cols, w, picked, out, rows, west, east):
    rows_per = own.shape[0]
    band = meta[0]
    core, odd = band % 2, (band // 2) % 2
    slot_of_near = jnp.where(odd == 1, 0, 2 * REACH)
    slot_of_far = 2 * REACH - slot_of_near
    slot_of_hop = jnp.where(core == 0, REACH - 1, REACH + 1)
    slot_of_mate = 2 * REACH - slot_of_hop

    def place(slot, tile, cols):
        rows[pl.ds(1 + slot * rows_per, rows_per)] = tile
        for i in range(rows_per):
            west[slot * rows_per + i] = cols[i : i + 1]
            east[slot * rows_per + i] = cols[rows_per + i : rows_per + i + 1]

    place(REACH, own[...], own_cols[...].astype(F32))
    place(slot_of_near, near[...], near_cols[...].astype(F32))
    place(slot_of_far, far[...], far_cols[...].astype(F32))
    place(slot_of_hop, mate[:rows_per], mate[2 * rows_per + 1].astype(F32))
    place(slot_of_mate, mate[rows_per : 2 * rows_per], mate[2 * rows_per + 2].astype(F32))
    last = (2 * REACH + 1) * rows_per + 1
    rows[jnp.where(core == 0, 0, last)] = beyond[0]
    rows[jnp.where(core == 0, last, 0)] = mate[2 * rows_per]

    @pl.when(band <= REACH)
    def _():
        edge = rows_per * (REACH - band)
        rows[edge] = rows[edge + 1]

    @pl.when(band >= meta[2] - 1 - REACH)
    def _():
        edge = rows_per * (meta[2] + REACH - band)
        rows[edge + 1] = rows[edge]

    lon, chan = own.shape[1], own.shape[2]
    cells = STRIP_ROWS * lon
    first_strip = (band - REACH) * (rows_per // STRIP_ROWS)
    place_in_row = lax.broadcasted_iota(jnp.int32, (STRIP_ROWS, lon, chan), 1)
    for k in range(SLOTS):
        base = STRIP_ROWS * (meta[4 + k] - first_strip)
        block = rows[pl.ds(base, STRIP_ROWS + 2)].astype(F32)
        centre = block[1:-1]
        north = (block[2:] - block[:-2]) * 0.5
        flat = centre.reshape(cells, chan)
        before = pltpu.roll(flat, 1, axis=0).reshape(centre.shape)
        after = pltpu.roll(flat, cells - 1, axis=0).reshape(centre.shape)
        before = jnp.where(place_in_row == 0, west[pl.ds(base, STRIP_ROWS)], before)
        after = jnp.where(place_in_row == lon - 1, east[pl.ds(base, STRIP_ROWS)], after)
        eastward = (after - before) * 0.5
        live = k < meta[3]
        for c, part in enumerate((centre, eastward, north)):
            start = (3 * k + c) * cells
            part = jnp.where(live, part.reshape(cells, chan), 0.0)
            picked[start : start + cells] = part.astype(BF16)
    out[...] = jnp.dot(w[...], picked[...], preferred_element_type=F32).astype(BF16)


def block_body(w, picked, out):
    out[...] = jnp.dot(w[...], picked[...], preferred_element_type=F32).astype(out.dtype)


def body(field, weights, strip_ids, counts):
    band, sector = lax.axis_index("lat"), lax.axis_index("lon")
    bands = lax.axis_size("lat")
    core, odd, parity = band % 2, (band // 2) % 2, sector % 2
    rows_per, lon, chan = field.shape
    near_lon = lambda i: i ^ 1
    far_lon = lambda i: (i + 1) % 8 if i % 2 else (i - 1) % 8

    far = swap(field, "lat", far_chip)
    near = swap(field, "lat", near_chip)
    edge_row = jnp.where(core == 1, field[-1:], field[:1])
    beyond = swap(edge_row, "lat", lambda i: (i + 3) % 16 if i % 2 else (i - 3) % 16)
    west_edge, east_edge = field[:, 0], field[:, -1]
    from_far = swap(jnp.where(parity == 0, west_edge, east_edge), "lon", far_lon)
    from_near = swap(jnp.where(parity == 0, east_edge, west_edge), "lon", near_lon)
    cols = jnp.where(
        parity == 0, jnp.concatenate([from_far, from_near]), jnp.concatenate([from_near, from_far])
    )
    far_cols = swap(cols, "lat", far_chip)
    near_cols = swap(cols, "lat", near_chip)
    pick_near = core == odd
    other_rows = jnp.where(
        core == 0,
        jnp.where(pick_near, far[-1:], near[-1:]),
        jnp.where(pick_near, far[:1], near[:1]),
    )
    message = jnp.concatenate(
        [
            jnp.where(pick_near, near, far),
            field,
            other_rows,
            jnp.where(pick_near, near_cols, far_cols)[None],
            cols[None],
        ]
    )
    mate = swap(message, "lat", lambda i: i ^ 1)

    meta = jnp.concatenate(
        [
            jnp.stack([band, parity, bands]).astype(jnp.int32),
            counts.astype(jnp.int32),
            strip_ids[0].astype(jnp.int32),
        ]
    )
    w = pltpu.with_memory_space_constraint(weights[0, 0], pltpu.HBM)
    size = w.shape[0] // 3
    width = w.shape[1]
    vmem = pl.BlockSpec(memory_space=pltpu.VMEM)
    smem = pl.BlockSpec(memory_space=pltpu.SMEM)
    held = lambda x: pltpu.with_memory_space_constraint(x, pltpu.VMEM)

    def load(which):
        return pl.pallas_call(
            lambda *refs: load_body(*refs, which=which),
            in_specs=[smem, pl.BlockSpec(memory_space=pltpu.HBM)],
            out_specs=vmem,
            out_shape=pltpu.VMEM((size, width), BF16),
            scratch_shapes=[pltpu.SemaphoreType.DMA],
            compiler_params=pltpu.CompilerParams(vmem_limit_bytes=1 << 20),
            cost_estimate=pl.CostEstimate(flops=1 << 32, transcendentals=0, bytes_accessed=2 * size * width),
            name="load",
        )(meta, w)

    w_far, w_near, w_own = held(load(0)), held(load(1)), held(load(2))
    halo = (2 * REACH + 1) * rows_per
    picked, to_far = pl.pallas_call(
        prep_body,
        in_specs=[smem] + [vmem] * 9,
        out_specs=[vmem, vmem],
        out_shape=[pltpu.VMEM((width, chan), BF16), pltpu.VMEM((size, chan), BF16)],
        scratch_shapes=[
            pltpu.VMEM((halo + 2, lon, chan), BF16),
            pltpu.VMEM((halo, 1, chan), F32),
            pltpu.VMEM((halo, 1, chan), F32),
        ],
        compiler_params=pltpu.CompilerParams(vmem_limit_bytes=16 << 20),
        name="prep",
    )(meta, field, near, far, mate, beyond, cols, near_cols, far_cols, w_far)
    picked = held(picked)

    def block(w_block, dtype, name):
        return pl.pallas_call(
            block_body,
            in_specs=[vmem, vmem],
            out_specs=vmem,
            out_shape=pltpu.VMEM((size, chan), dtype),
            compiler_params=pltpu.CompilerParams(vmem_limit_bytes=16 << 20),
            name=name,
        )(w_block, picked)

    got_far = swap(to_far, "lon", far_lon)
    got_near = swap(block(w_near, BF16, "side"), "lon", near_lon)
    own = block(w_own, F32, "own")
    return (own + got_far.astype(F32) + got_near.astype(F32)).astype(BF16)


def solution(mesh):
    placed = (P("lat", "lon", None), P("lat", "lon", None, None), P("lat", None), P("lat"))
    return jax.shard_map(
        body, mesh=mesh, in_specs=placed, out_specs=P(("lat", "lon"), None), check_vma=False
    )
```

```python
import jax
import jax.numpy as jnp
from jax import lax
from jax.experimental import pallas as pl
from jax.experimental.pallas import tpu as pltpu
from jax.sharding import PartitionSpec as P

STRIP_ROWS = 4
SLOTS = 8
REACH = 2
CHUNKS = 4
BF16 = jnp.bfloat16
F32 = jnp.float32


def swap(block, axis, partner):
    return lax.ppermute(block, axis, [(i, partner(i)) for i in range(lax.axis_size(axis))])


def near_chip(i):
    return i ^ 2


def inside(to, spare, count=16):
    return to if 0 <= to < count else spare


def far_chip(i):
    return inside(i + 2 if (i // 2) % 2 else i - 2, i ^ 1)


def edges_body(field, tile, far_edge, near_edge, edge_row):
    core, parity = lax.axis_index("lat") % 2, lax.axis_index("lon") % 2
    tile[...] = field[...]
    last = field.shape[1] - 1
    for i in range(field.shape[0]):
        west, east = field[i, :1], field[i, last:]
        far_edge[i : i + 1] = jnp.where(parity == 0, west, east)
        near_edge[i : i + 1] = jnp.where(parity == 0, east, west)
    edge_row[...] = jnp.where(core == 1, field[-1:], field[:1])


def load_body(w, block, sem, *, far):
    parity = lax.axis_index("lon") % 2
    size = block.shape[0]
    start = jnp.where(parity == (0 if far else 1), 0, 2 * size)
    copy = pltpu.make_async_copy(w.at[pl.ds(start, size)], block, sem)
    copy.start()
    copy.wait()


def prep_body(ids, counts, own, near, far, mate, beyond, own_cols, near_cols, far_cols, w, picked, out, rows, west, east):
    rows_per = own.shape[0]
    band = lax.axis_index("lat")
    bands = lax.axis_size("lat")
    core, odd = band % 2, (band // 2) % 2
    slot_of_near = jnp.where(odd == 1, 0, 2 * REACH)
    slot_of_far = 2 * REACH - slot_of_near
    slot_of_hop = jnp.where(core == 0, REACH - 1, REACH + 1)
    slot_of_mate = 2 * REACH - slot_of_hop

    def place(slot, tile, cols):
        rows[pl.ds(1 + slot * rows_per, rows_per)] = tile
        for i in range(rows_per):
            west[slot * rows_per + i] = cols[i : i + 1]
            east[slot * rows_per + i] = cols[rows_per + i : rows_per + i + 1]

    place(REACH, own[...], own_cols[...].astype(F32))
    place(slot_of_near, near[...], near_cols[...].astype(F32))
    place(slot_of_far, far[...], far_cols[...].astype(F32))
    place(slot_of_hop, mate[:rows_per], mate[2 * rows_per + 1].astype(F32))
    place(slot_of_mate, mate[rows_per : 2 * rows_per], mate[2 * rows_per + 2].astype(F32))
    last = (2 * REACH + 1) * rows_per + 1
    rows[jnp.where(core == 0, 0, last)] = beyond[0]
    rows[jnp.where(core == 0, last, 0)] = mate[2 * rows_per]

    @pl.when(band <= REACH)
    def _():
        edge = rows_per * (REACH - band)
        rows[edge] = rows[edge + 1]

    @pl.when(band >= bands - 1 - REACH)
    def _():
        edge = rows_per * (bands + REACH - band)
        rows[edge + 1] = rows[edge]

    lon, chan = own.shape[1], own.shape[2]
    cells = STRIP_ROWS * lon
    first_strip = (band - REACH) * (rows_per // STRIP_ROWS)
    place_in_row = lax.broadcasted_iota(jnp.int32, (STRIP_ROWS, lon, chan), 1)
    for k in range(SLOTS):
        base = STRIP_ROWS * (ids[0, k] - first_strip)
        block = rows[pl.ds(base, STRIP_ROWS + 2)].astype(F32)
        centre = block[1:-1]
        north = (block[2:] - block[:-2]) * 0.5
        flat = centre.reshape(cells, chan)
        before = pltpu.roll(flat, 1, axis=0).reshape(centre.shape)
        after = pltpu.roll(flat, cells - 1, axis=0).reshape(centre.shape)
        before = jnp.where(place_in_row == 0, west[pl.ds(base, STRIP_ROWS)], before)
        after = jnp.where(place_in_row == lon - 1, east[pl.ds(base, STRIP_ROWS)], after)
        eastward = (after - before) * 0.5
        live = k < counts[0]
        for c, part in enumerate((centre, eastward, north)):
            start = (3 * k + c) * cells
            part = jnp.where(live, part.reshape(cells, chan), 0.0)
            picked[start : start + cells] = part.astype(BF16)
    out[...] = jnp.dot(w[...], picked[...], preferred_element_type=F32).astype(BF16)


def side_body(w, picked, out):
    out[...] = jnp.dot(w[...], picked[...], preferred_element_type=F32).astype(BF16)


def own_body(w, picked, out, held, sems):
    size = out.shape[0]
    part = size // CHUNKS
    copies = [
        pltpu.make_async_copy(
            w.at[pl.ds(size + part * c, part)], held.at[pl.ds(part * c, part)], sems.at[c]
        )
        for c in range(CHUNKS)
    ]
    for copy in copies:
        copy.start()
    for c, copy in enumerate(copies):
        copy.wait()
        here = slice(part * c, part * (c + 1))
        out[here] = jnp.dot(held[here], picked[...], preferred_element_type=F32)


def remap(field, weights, strip_ids, counts):
    band, sector = lax.axis_index("lat"), lax.axis_index("lon")
    core, odd, parity = band % 2, (band // 2) % 2, sector % 2
    rows_per, lon, chan = field.shape
    near_lon = lambda i: i ^ 1
    far_lon = lambda i: (i + 1) % 8 if i % 2 else (i - 1) % 8
    vmem = pl.BlockSpec(memory_space=pltpu.VMEM)
    smem = pl.BlockSpec(memory_space=pltpu.SMEM)
    hbm = pl.BlockSpec(memory_space=pltpu.HBM)
    held = lambda x: pltpu.with_memory_space_constraint(x, pltpu.VMEM)
    small = pltpu.CompilerParams(vmem_limit_bytes=2 << 20)

    tile, far_edge, near_edge, edge_row = pl.pallas_call(
        edges_body,
        in_specs=[vmem],
        out_specs=[vmem] * 4,
        out_shape=[
            pltpu.VMEM(field.shape, BF16),
            pltpu.VMEM((rows_per, chan), BF16),
            pltpu.VMEM((rows_per, chan), BF16),
            pltpu.VMEM((1, lon, chan), BF16),
        ],
        compiler_params=small,
        name="edges",
    )(field)
    far = swap(tile, "lat", far_chip)
    near = swap(tile, "lat", near_chip)
    from_far = swap(far_edge, "lon", far_lon)
    from_near = swap(near_edge, "lon", near_lon)
    beyond = swap(edge_row, "lat", lambda i: inside(i + 3 if i % 2 else i - 3, i ^ 2))
    cols = jnp.where(
        parity == 0, jnp.concatenate([from_far, from_near]), jnp.concatenate([from_near, from_far])
    )
    far_cols = swap(cols, "lat", far_chip)
    near_cols = swap(cols, "lat", near_chip)

    w = pltpu.with_memory_space_constraint(weights[0, 0], pltpu.HBM)
    size = w.shape[0] // 3
    width = w.shape[1]

    def load(far):
        return pl.pallas_call(
            lambda *refs: load_body(*refs, far=far),
            in_specs=[hbm],
            out_specs=vmem,
            out_shape=pltpu.VMEM((size, width), BF16),
            scratch_shapes=[pltpu.SemaphoreType.DMA],
            compiler_params=small,
        )(w)

    w_far, w_near = load(True), load(False)

    pick_near = core == odd
    other_rows = jnp.where(
        core == 0,
        jnp.where(pick_near, far[-1:], near[-1:]),
        jnp.where(pick_near, far[:1], near[:1]),
    )
    message = jnp.concatenate(
        [
            jnp.where(pick_near, near, far),
            tile,
            other_rows,
            jnp.where(pick_near, near_cols, far_cols)[None],
            cols[None],
        ]
    )
    mate = swap(message, "lat", lambda i: i ^ 1)

    halo = (2 * REACH + 1) * rows_per
    picked, to_far = pl.pallas_call(
        prep_body,
        in_specs=[smem, smem] + [vmem] * 9,
        out_specs=[vmem, vmem],
        out_shape=[pltpu.VMEM((width, chan), BF16), pltpu.VMEM((size, chan), BF16)],
        scratch_shapes=[
            pltpu.VMEM((halo + 2, lon, chan), BF16),
            pltpu.VMEM((halo, 1, chan), F32),
            pltpu.VMEM((halo, 1, chan), F32),
        ],
        compiler_params=pltpu.CompilerParams(vmem_limit_bytes=16 << 20),
        name="prep",
    )(strip_ids, counts, held(tile), near, far, mate, beyond, cols, near_cols, far_cols, held(w_far))
    picked = held(picked)
    got_far = swap(to_far, "lon", far_lon)
    to_near = pl.pallas_call(
        side_body,
        in_specs=[vmem, vmem],
        out_specs=vmem,
        out_shape=pltpu.VMEM((size, chan), BF16),
        compiler_params=pltpu.CompilerParams(vmem_limit_bytes=16 << 20),
        name="side",
    )(held(w_near), picked)
    got_near = swap(to_near, "lon", near_lon)
    own = pl.pallas_call(
        own_body,
        in_specs=[hbm, vmem],
        out_specs=vmem,
        out_shape=pltpu.VMEM((size, chan), F32),
        scratch_shapes=[pltpu.VMEM((size, width), BF16), pltpu.SemaphoreType.DMA((CHUNKS,))],
        compiler_params=pltpu.CompilerParams(vmem_limit_bytes=16 << 20),
        name="own",
    )(w, picked)
    return (own + got_far.astype(F32) + got_near.astype(F32)).astype(BF16)


def solution(mesh):
    placed = (P("lat", "lon", None), P("lat", "lon", None, None), P("lat", None), P("lat"))
    return jax.shard_map(
        remap, mesh=mesh, in_specs=placed, out_specs=P(("lat", "lon"), None), check_vma=False
    )
```

```python
import jax
import jax.numpy as jnp
from jax import lax
from jax.experimental import pallas as pl
from jax.experimental.pallas import tpu as pltpu
from jax.sharding import PartitionSpec as P

STRIP_ROWS = 4
SLOTS = 8
REACH = 2
CHUNKS = 4
BF16 = jnp.bfloat16
F32 = jnp.float32


def swap(block, axis, partner):
    return lax.ppermute(block, axis, [(i, partner(i)) for i in range(lax.axis_size(axis))])


def near_chip(i):
    return i ^ 2


def inside(to, spare, count=16):
    return to if 0 <= to < count else spare


def far_chip(i):
    return inside(i + 2 if (i // 2) % 2 else i - 2, i ^ 1)


def edges_body(field, tile, far_edge, near_edge, edge_row):
    core, parity = lax.axis_index("lat") % 2, lax.axis_index("lon") % 2
    tile[...] = field[...]
    last = field.shape[1] - 1
    for i in range(field.shape[0]):
        west, east = field[i, :1], field[i, last:]
        far_edge[i : i + 1] = jnp.where(parity == 0, west, east)
        near_edge[i : i + 1] = jnp.where(parity == 0, east, west)
    edge_row[...] = jnp.where(core == 1, field[-1:], field[:1])


def rows_of(w, far, first, count):
    even = lax.axis_index("lon") % 2 == 0
    top = jnp.where(even, 0, 2 * w.shape[0] // 3) if far else jnp.where(even, 2 * w.shape[0] // 3, 0)
    return w.at[pl.ds(top + first, count)]


def load_body(w, far, sem):
    half = far.shape[0] // 2
    copy = pltpu.make_async_copy(rows_of(w, True, 0, half), far.at[pl.ds(0, half)], sem)
    copy.start()
    copy.wait()


def more_body(w, _, far, near, sems):
    half = far.shape[0] // 2
    copies = (
        pltpu.make_async_copy(rows_of(w, True, half, half), far.at[pl.ds(half, half)], sems.at[0]),
        pltpu.make_async_copy(rows_of(w, False, 0, half), near.at[pl.ds(0, half)], sems.at[1]),
    )
    for copy in copies:
        copy.start()
    for copy in copies:
        copy.wait()


def prep_body(ids, counts, own, near, far, mate, beyond, own_cols, near_cols, far_cols, w, w_all, _, picked, out, w_near, rows, west, east, sem):
    half = w_near.shape[0] // 2
    coming = pltpu.make_async_copy(rows_of(w_all, False, half, half), w_near.at[pl.ds(half, half)], sem)
    coming.start()
    rows_per = own.shape[0]
    band = lax.axis_index("lat")
    bands = lax.axis_size("lat")
    core, odd = band % 2, (band // 2) % 2
    slot_of_near = jnp.where(odd == 1, 0, 2 * REACH)
    slot_of_far = 2 * REACH - slot_of_near
    slot_of_hop = jnp.where(core == 0, REACH - 1, REACH + 1)
    slot_of_mate = 2 * REACH - slot_of_hop

    def place(slot, tile, cols):
        rows[pl.ds(1 + slot * rows_per, rows_per)] = tile
        for i in range(rows_per):
            west[slot * rows_per + i] = cols[i : i + 1]
            east[slot * rows_per + i] = cols[rows_per + i : rows_per + i + 1]

    place(REACH, own[...], own_cols[...].astype(F32))
    place(slot_of_near, near[...], near_cols[...].astype(F32))
    place(slot_of_far, far[...], far_cols[...].astype(F32))
    place(slot_of_hop, mate[:rows_per], mate[2 * rows_per + 1].astype(F32))
    place(slot_of_mate, mate[rows_per : 2 * rows_per], mate[2 * rows_per + 2].astype(F32))
    last = (2 * REACH + 1) * rows_per + 1
    rows[jnp.where(core == 0, 0, last)] = beyond[0]
    rows[jnp.where(core == 0, last, 0)] = mate[2 * rows_per]

    @pl.when(band <= REACH)
    def _():
        edge = rows_per * (REACH - band)
        rows[edge] = rows[edge + 1]

    @pl.when(band >= bands - 1 - REACH)
    def _():
        edge = rows_per * (bands + REACH - band)
        rows[edge + 1] = rows[edge]

    lon, chan = own.shape[1], own.shape[2]
    cells = STRIP_ROWS * lon
    first_strip = (band - REACH) * (rows_per // STRIP_ROWS)
    place_in_row = lax.broadcasted_iota(jnp.int32, (STRIP_ROWS, lon, chan), 1)
    for k in range(SLOTS):
        base = STRIP_ROWS * (ids[0, k] - first_strip)
        block = rows[pl.ds(base, STRIP_ROWS + 2)].astype(F32)
        centre = block[1:-1]
        north = (block[2:] - block[:-2]) * 0.5
        flat = centre.reshape(cells, chan)
        before = pltpu.roll(flat, 1, axis=0).reshape(centre.shape)
        after = pltpu.roll(flat, cells - 1, axis=0).reshape(centre.shape)
        before = jnp.where(place_in_row == 0, west[pl.ds(base, STRIP_ROWS)], before)
        after = jnp.where(place_in_row == lon - 1, east[pl.ds(base, STRIP_ROWS)], after)
        eastward = (after - before) * 0.5
        live = k < counts[0]
        for c, part in enumerate((centre, eastward, north)):
            start = (3 * k + c) * cells
            part = jnp.where(live, part.reshape(cells, chan), 0.0)
            picked[start : start + cells] = part.astype(BF16)
    out[...] = jnp.dot(w[...], picked[...], preferred_element_type=F32).astype(BF16)
    coming.wait()


def side_body(w, picked, out):
    out[...] = jnp.dot(w[...], picked[...], preferred_element_type=F32).astype(BF16)


def own_body(w, picked, out, held, sems):
    size = out.shape[0]
    part = size // CHUNKS
    copies = [
        pltpu.make_async_copy(
            w.at[pl.ds(size + part * c, part)], held.at[pl.ds(part * c, part)], sems.at[c]
        )
        for c in range(CHUNKS)
    ]
    for copy in copies:
        copy.start()
    for c, copy in enumerate(copies):
        copy.wait()
        here = slice(part * c, part * (c + 1))
        out[here] = jnp.dot(held[here], picked[...], preferred_element_type=F32)


def remap(field, weights, strip_ids, counts):
    band, sector = lax.axis_index("lat"), lax.axis_index("lon")
    core, odd, parity = band % 2, (band // 2) % 2, sector % 2
    rows_per, lon, chan = field.shape
    near_lon = lambda i: i ^ 1
    far_lon = lambda i: (i + 1) % 8 if i % 2 else (i - 1) % 8
    vmem = pl.BlockSpec(memory_space=pltpu.VMEM)
    smem = pl.BlockSpec(memory_space=pltpu.SMEM)
    hbm = pl.BlockSpec(memory_space=pltpu.HBM)
    held = lambda x: pltpu.with_memory_space_constraint(x, pltpu.VMEM)
    small = pltpu.CompilerParams(vmem_limit_bytes=2 << 20)

    tile, far_edge, near_edge, edge_row = pl.pallas_call(
        edges_body,
        in_specs=[vmem],
        out_specs=[vmem] * 4,
        out_shape=[
            pltpu.VMEM(field.shape, BF16),
            pltpu.VMEM((rows_per, chan), BF16),
            pltpu.VMEM((rows_per, chan), BF16),
            pltpu.VMEM((1, lon, chan), BF16),
        ],
        compiler_params=small,
        name="edges",
    )(field)
    far = swap(tile, "lat", far_chip)
    near = swap(tile, "lat", near_chip)
    from_far = swap(far_edge, "lon", far_lon)
    from_near = swap(near_edge, "lon", near_lon)
    beyond = swap(edge_row, "lat", lambda i: inside(i + 3 if i % 2 else i - 3, i ^ 2))
    cols = jnp.where(
        parity == 0, jnp.concatenate([from_far, from_near]), jnp.concatenate([from_near, from_far])
    )
    far_cols = swap(cols, "lat", far_chip)
    near_cols = swap(cols, "lat", near_chip)

    w = pltpu.with_memory_space_constraint(weights[0, 0], pltpu.HBM)
    size = w.shape[0] // 3
    width = w.shape[1]

    block = pltpu.VMEM((size, width), BF16)
    w_far = pl.pallas_call(
        load_body,
        in_specs=[hbm],
        out_specs=vmem,
        out_shape=block,
        scratch_shapes=[pltpu.SemaphoreType.DMA],
        compiler_params=small,
        name="load_far",
    )(w)
    w_far, w_near = pl.pallas_call(
        more_body,
        in_specs=[hbm, vmem],
        out_specs=[vmem, vmem],
        out_shape=[block, block],
        scratch_shapes=[pltpu.SemaphoreType.DMA((2,))],
        input_output_aliases={1: 0},
        compiler_params=small,
        name="load_more",
    )(w, held(w_far))

    pick_near = core == odd
    other_rows = jnp.where(
        core == 0,
        jnp.where(pick_near, far[-1:], near[-1:]),
        jnp.where(pick_near, far[:1], near[:1]),
    )
    message = jnp.concatenate(
        [
            jnp.where(pick_near, near, far),
            tile,
            other_rows,
            jnp.where(pick_near, near_cols, far_cols)[None],
            cols[None],
        ]
    )
    mate = swap(message, "lat", lambda i: i ^ 1)

    halo = (2 * REACH + 1) * rows_per
    picked, to_far, w_near = pl.pallas_call(
        prep_body,
        in_specs=[smem, smem] + [vmem] * 9 + [hbm, vmem],
        input_output_aliases={12: 2},
        out_specs=[vmem] * 3,
        out_shape=[
            pltpu.VMEM((width, chan), BF16),
            pltpu.VMEM((size, chan), BF16),
            pltpu.VMEM((size, width), BF16),
        ],
        scratch_shapes=[
            pltpu.VMEM((halo + 2, lon, chan), BF16),
            pltpu.VMEM((halo, 1, chan), F32),
            pltpu.VMEM((halo, 1, chan), F32),
            pltpu.SemaphoreType.DMA,
        ],
        compiler_params=pltpu.CompilerParams(vmem_limit_bytes=16 << 20),
        name="prep",
    )(strip_ids, counts, held(tile), near, far, mate, beyond, cols, near_cols, far_cols, held(w_far), w, held(w_near))
    picked = held(picked)
    got_far = swap(to_far, "lon", far_lon)
    to_near = pl.pallas_call(
        side_body,
        in_specs=[vmem, vmem],
        out_specs=vmem,
        out_shape=pltpu.VMEM((size, chan), BF16),
        compiler_params=pltpu.CompilerParams(vmem_limit_bytes=16 << 20),
        name="side",
    )(held(w_near), picked)
    got_near = swap(to_near, "lon", near_lon)
    own = pl.pallas_call(
        own_body,
        in_specs=[hbm, vmem],
        out_specs=vmem,
        out_shape=pltpu.VMEM((size, chan), F32),
        scratch_shapes=[pltpu.VMEM((size, width), BF16), pltpu.SemaphoreType.DMA((CHUNKS,))],
        compiler_params=pltpu.CompilerParams(vmem_limit_bytes=16 << 20),
        name="own",
    )(w, picked)
    return (own + got_far.astype(F32) + got_near.astype(F32)).astype(BF16)


def solution(mesh):
    placed = (P("lat", "lon", None), P("lat", "lon", None, None), P("lat", None), P("lat"))
    return jax.shard_map(
        remap, mesh=mesh, in_specs=placed, out_specs=P(("lat", "lon"), None), check_vma=False
    )
```

```python
import jax
import jax.numpy as jnp
from jax import lax
from jax.experimental import pallas as pl
from jax.experimental.pallas import tpu as pltpu
from jax.sharding import PartitionSpec as P

STRIP_ROWS = 4
SLOTS = 8
REACH = 2
CHUNKS = 4
LEAD = 320
EARLY = 384
BF16 = jnp.bfloat16
F32 = jnp.float32


def swap(block, axis, partner):
    return lax.ppermute(block, axis, [(i, partner(i)) for i in range(lax.axis_size(axis))])


def near_chip(i):
    return i ^ 2


def inside(to, spare, count=16):
    return to if 0 <= to < count else spare


def far_chip(i):
    return inside(i + 2 if (i // 2) % 2 else i - 2, i ^ 1)


def edges_body(field, tile, far_edge, near_edge, edge_row):
    core, parity = lax.axis_index("lat") % 2, lax.axis_index("lon") % 2
    tile[...] = field[...]
    last = field.shape[1] - 1
    for i in range(field.shape[0]):
        west, east = field[i, :1], field[i, last:]
        far_edge[i : i + 1] = jnp.where(parity == 0, west, east)
        near_edge[i : i + 1] = jnp.where(parity == 0, east, west)
    edge_row[...] = jnp.where(core == 1, field[-1:], field[:1])


def rows_of(w, far, first, count):
    even = lax.axis_index("lon") % 2 == 0
    top = jnp.where(even, 0, 2 * w.shape[0] // 3) if far else jnp.where(even, 2 * w.shape[0] // 3, 0)
    return w.at[pl.ds(top + first, count)]


def load_body(w, far, near, sems):
    copies = (
        pltpu.make_async_copy(rows_of(w, True, 0, far.shape[0]), far, sems.at[0]),
        pltpu.make_async_copy(rows_of(w, False, 0, EARLY), near.at[pl.ds(0, EARLY)], sems.at[1]),
    )
    for copy in copies:
        copy.start()
    for copy in copies:
        copy.wait()


def prep_body(ids, counts, own, near, far, hop, mate, beyond, own_cols, near_cols, far_cols, w, w_all, _, picked, out, w_near, rows, west, east, sem):
    late = w_near.shape[0] - EARLY
    coming = pltpu.make_async_copy(rows_of(w_all, False, EARLY, late), w_near.at[pl.ds(EARLY, late)], sem)
    coming.start()
    rows_per = own.shape[0]
    band = lax.axis_index("lat")
    bands = lax.axis_size("lat")
    core, odd = band % 2, (band // 2) % 2
    slot_of_near = jnp.where(odd == 1, 0, 2 * REACH)
    slot_of_far = 2 * REACH - slot_of_near
    slot_of_hop = jnp.where(core == 0, REACH - 1, REACH + 1)
    slot_of_mate = 2 * REACH - slot_of_hop

    def place(slot, tile, cols):
        rows[pl.ds(1 + slot * rows_per, rows_per)] = tile
        for i in range(rows_per):
            west[slot * rows_per + i] = cols[i : i + 1]
            east[slot * rows_per + i] = cols[rows_per + i : rows_per + i + 1]

    place(REACH, own[...], own_cols[...].astype(F32))
    place(slot_of_near, near[...], near_cols[...].astype(F32))
    place(slot_of_far, far[...], far_cols[...].astype(F32))
    place(slot_of_hop, hop[:rows_per], hop[rows_per + 1].astype(F32))
    place(slot_of_mate, mate[...], hop[rows_per + 2].astype(F32))
    last = (2 * REACH + 1) * rows_per + 1
    rows[jnp.where(core == 0, 0, last)] = beyond[0]
    rows[jnp.where(core == 0, last, 0)] = hop[rows_per]

    @pl.when(band <= REACH)
    def _():
        edge = rows_per * (REACH - band)
        rows[edge] = rows[edge + 1]

    @pl.when(band >= bands - 1 - REACH)
    def _():
        edge = rows_per * (bands + REACH - band)
        rows[edge + 1] = rows[edge]

    lon, chan = own.shape[1], own.shape[2]
    cells = STRIP_ROWS * lon
    first_strip = (band - REACH) * (rows_per // STRIP_ROWS)
    place_in_row = lax.broadcasted_iota(jnp.int32, (STRIP_ROWS, lon, chan), 1)
    for k in range(SLOTS):
        base = STRIP_ROWS * (ids[0, k] - first_strip)
        block = rows[pl.ds(base, STRIP_ROWS + 2)].astype(F32)
        centre = block[1:-1]
        north = (block[2:] - block[:-2]) * 0.5
        flat = centre.reshape(cells, chan)
        before = pltpu.roll(flat, 1, axis=0).reshape(centre.shape)
        after = pltpu.roll(flat, cells - 1, axis=0).reshape(centre.shape)
        before = jnp.where(place_in_row == 0, west[pl.ds(base, STRIP_ROWS)], before)
        after = jnp.where(place_in_row == lon - 1, east[pl.ds(base, STRIP_ROWS)], after)
        eastward = (after - before) * 0.5
        live = k < counts[0]
        for c, part in enumerate((centre, eastward, north)):
            start = (3 * k + c) * cells
            part = jnp.where(live, part.reshape(cells, chan), 0.0)
            picked[start : start + cells] = part.astype(BF16)
    out[...] = jnp.dot(w[...], picked[...], preferred_element_type=F32).astype(BF16)
    coming.wait()


def side_body(w, picked, out, *, first):
    out[...] = jnp.dot(
        w[first : first + out.shape[0]], picked[...], preferred_element_type=F32
    ).astype(BF16)


def own_body(w, picked, out, held, sems):
    size = out.shape[0]
    part = size // CHUNKS
    copies = [
        pltpu.make_async_copy(
            w.at[pl.ds(size + part * c, part)], held.at[pl.ds(part * c, part)], sems.at[c]
        )
        for c in range(CHUNKS)
    ]
    for copy in copies:
        copy.start()
    for c, copy in enumerate(copies):
        copy.wait()
        here = slice(part * c, part * (c + 1))
        out[here] = jnp.dot(held[here], picked[...], preferred_element_type=F32)


def join_body(own, far, near_a, near_b, out, ready, sems):
    copies = []
    for c, (first, near) in enumerate(((0, near_a), (LEAD, near_b))):
        here = slice(first, first + near.shape[0])
        ready[here] = (own[here] + far[here].astype(F32) + near[...].astype(F32)).astype(BF16)
        span = pl.ds(first, near.shape[0])
        copies.append(pltpu.make_async_copy(ready.at[span], out.at[span], sems.at[c]))
        copies[-1].start()
    for copy in copies:
        copy.wait()


def remap(field, weights, strip_ids, counts):
    band, sector = lax.axis_index("lat"), lax.axis_index("lon")
    core, odd, parity = band % 2, (band // 2) % 2, sector % 2
    rows_per, lon, chan = field.shape
    near_lon = lambda i: i ^ 1
    far_lon = lambda i: (i + 1) % 8 if i % 2 else (i - 1) % 8
    vmem = pl.BlockSpec(memory_space=pltpu.VMEM)
    smem = pl.BlockSpec(memory_space=pltpu.SMEM)
    hbm = pl.BlockSpec(memory_space=pltpu.HBM)
    held = lambda x: pltpu.with_memory_space_constraint(x, pltpu.VMEM)
    small = pltpu.CompilerParams(vmem_limit_bytes=2 << 20)

    tile, far_edge, near_edge, edge_row = pl.pallas_call(
        edges_body,
        in_specs=[vmem],
        out_specs=[vmem] * 4,
        out_shape=[
            pltpu.VMEM(field.shape, BF16),
            pltpu.VMEM((rows_per, chan), BF16),
            pltpu.VMEM((rows_per, chan), BF16),
            pltpu.VMEM((1, lon, chan), BF16),
        ],
        compiler_params=small,
        name="edges",
    )(field)
    far = swap(tile, "lat", far_chip)
    near = swap(tile, "lat", near_chip)
    from_far = swap(far_edge, "lon", far_lon)
    from_near = swap(near_edge, "lon", near_lon)
    beyond = swap(edge_row, "lat", lambda i: inside(i + 3 if i % 2 else i - 3, i ^ 2))
    cols = jnp.where(
        parity == 0, jnp.concatenate([from_far, from_near]), jnp.concatenate([from_near, from_far])
    )
    far_cols = swap(cols, "lat", far_chip)
    near_cols = swap(cols, "lat", near_chip)

    w = pltpu.with_memory_space_constraint(weights[0, 0], pltpu.HBM)
    size = w.shape[0] // 3
    width = w.shape[1]

    block = pltpu.VMEM((size, width), BF16)
    w_far, w_near = pl.pallas_call(
        load_body,
        in_specs=[hbm],
        out_specs=[vmem, vmem],
        out_shape=[block, block],
        scratch_shapes=[pltpu.SemaphoreType.DMA((2,))],
        compiler_params=small,
        name="load",
    )(w)

    mate = swap(tile, "lat", lambda i: i ^ 1)
    pick_near = core == odd
    other_rows = jnp.where(
        core == 0,
        jnp.where(pick_near, far[-1:], near[-1:]),
        jnp.where(pick_near, far[:1], near[:1]),
    )
    message = jnp.concatenate(
        [
            jnp.where(pick_near, near, far),
            other_rows,
            jnp.where(pick_near, near_cols, far_cols)[None],
            cols[None],
        ]
    )
    hop = swap(message, "lat", lambda i: i ^ 1)

    halo = (2 * REACH + 1) * rows_per
    picked, to_far, w_near = pl.pallas_call(
        prep_body,
        in_specs=[smem, smem] + [vmem] * 10 + [hbm, vmem],
        input_output_aliases={13: 2},
        out_specs=[vmem] * 3,
        out_shape=[
            pltpu.VMEM((width, chan), BF16),
            pltpu.VMEM((size, chan), BF16),
            pltpu.VMEM((size, width), BF16),
        ],
        scratch_shapes=[
            pltpu.VMEM((halo + 2, lon, chan), BF16),
            pltpu.VMEM((halo, 1, chan), F32),
            pltpu.VMEM((halo, 1, chan), F32),
            pltpu.SemaphoreType.DMA,
        ],
        compiler_params=pltpu.CompilerParams(vmem_limit_bytes=16 << 20),
        name="prep",
    )(strip_ids, counts, held(tile), near, far, hop, mate, beyond, cols, near_cols, far_cols, held(w_far), w, held(w_near))
    picked = held(picked)
    got_far = swap(to_far, "lon", far_lon)
    w_near = held(w_near)

    def side(first, count):
        return pl.pallas_call(
            lambda *refs: side_body(*refs, first=first),
            in_specs=[vmem, vmem],
            out_specs=vmem,
            out_shape=pltpu.VMEM((count, chan), BF16),
            compiler_params=pltpu.CompilerParams(vmem_limit_bytes=16 << 20),
        )(w_near, picked)

    got_near = [
        swap(side(0, LEAD), "lon", near_lon), swap(side(LEAD, size - LEAD), "lon", near_lon)
    ]
    own = pl.pallas_call(
        own_body,
        in_specs=[hbm, vmem],
        out_specs=vmem,
        out_shape=pltpu.VMEM((size, chan), F32),
        scratch_shapes=[pltpu.VMEM((size, width), BF16), pltpu.SemaphoreType.DMA((CHUNKS,))],
        compiler_params=pltpu.CompilerParams(vmem_limit_bytes=16 << 20),
        name="own",
    )(w, picked)
    return pl.pallas_call(
        join_body,
        in_specs=[vmem] * 4,
        out_specs=hbm,
        out_shape=jax.ShapeDtypeStruct((size, chan), BF16),
        scratch_shapes=[pltpu.VMEM((size, chan), BF16), pltpu.SemaphoreType.DMA((2,))],
        compiler_params=pltpu.CompilerParams(vmem_limit_bytes=4 << 20),
        name="join",
    )(held(own), got_far, *got_near)


def solution(mesh):
    placed = (P("lat", "lon", None), P("lat", "lon", None, None), P("lat", None), P("lat"))
    return jax.shard_map(
        remap, mesh=mesh, in_specs=placed, out_specs=P(("lat", "lon"), None), check_vma=False
    )
```
